128 devices in a mesh: grp: 32 (over y, z_hi, x), sub: 4 (over z_lo, core).
Axes of the slice: x: 4, y: 4, z: 4 (z_hi: 2, z_lo: 2; z = z_hi * 2 + z_lo), core: 2. Of those that a mesh axis runs over, the one named last changes fastest.
Arguments:
- master: float32 [16384, 3584], P(('grp', 'sub')), may hold values from -120 to 120
- moment_one: float32 [16384, 3584], P(('grp', 'sub')), may hold values from -6 to 6
- moment_two: float32 [16384, 3584], P(('grp', 'sub')), may hold values from 0.01 to 4
- gradient: float32 [16384, 3584], P(('grp', 'sub')), may hold values from -120 to 120
- partner: int32 [128], replicated, may hold values from 0 to 127, each once
- tensor_of_row: int32 [16384], replicated, may hold values from 0 to 7, never falling along the last dimension, each value on 1 to 4096 neighbouring positions
Outputs:
- new_master: float32 [16384, 3584], P(('grp', 'sub'))
- new_moment_one: float32 [16384, 3584], P(('grp', 'sub'))
- new_moment_two: float32 [16384, 3584], P(('grp', 'sub'))
The draws below stay inside these ranges and needn't reach their ends.
Inputs may be any that keep to these rules, and one draw needn't show every extreme that they name: partner[n] is the device of new rank n; every device holds exactly one rank. `tensor_of_row`: tensor numbers never fall along the rows; each of the 8 tensors has one or more rows.
All inputs are finite; a program needn't handle non-finite values.
Results may differ from the reference program's by a relative error of at most 0.00007.
Values sent between devices are 32-bit elements; how exact they have to be, the bound alone decides.
No kernel may reach another device: no remote copies, remote signals or barrier semaphores. Data moves between devices by JAX's collectives and lax.ppermute only.
A program may use at most 128 MiB of HBM per device.

```python
import math
import jax
import jax.numpy as jnp
import numpy as np
from jax import lax

W = 3584
ROWS_DEV = 128
LAYERS = 8
NDEV = 128
ROWS = 16384
BLOCK = 1


def scale_field(key, trend_pos):
    key_row, key_col = jax.random.split(key, 2)
    row_scale = jnp.exp(jax.random.uniform(key_row, (ROWS, 1), jnp.float32, 0.0, math.log(10.0)))
    col_scale = jnp.exp(jax.random.uniform(key_col, (1, W), jnp.float32, 0.0, math.log(10.0)))
    trend = jnp.power(3.0, trend_pos.astype(jnp.float32) / max(NDEV - 1, 1))
    return row_scale * col_scale * trend[:, None] / 15.0


def draw_master(key, part):
    key = jax.random.fold_in(key, 11)
    key_scale, key_noise = jax.random.split(key, 2)
    row_index = jnp.arange(ROWS, dtype=jnp.int32)
    trend_pos = row_index % ROWS_DEV // BLOCK
    noise = jax.random.normal(key_noise, (ROWS, W), jnp.float32)
    noise = jnp.clip(noise, -6.0, 6.0)
    return noise * scale_field(key_scale, trend_pos)


def draw_gradient(key, part):
    key = jax.random.fold_in(key, 23)
    key_scale, key_noise = jax.random.split(key, 2)
    row_index = jnp.arange(ROWS, dtype=jnp.int32)
    trend_pos = row_index // ROWS_DEV
    noise = jax.random.normal(key_noise, (ROWS, W), jnp.float32)
    noise = jnp.clip(noise, -6.0, 6.0)
    return noise * scale_field(key_scale, trend_pos)


def steps_of(rng, dims, pieces, smallest, top_value):
    gain, own = 1.0, jax.random.fold_in(rng, 6)
    for dim, shards_of in pieces:
        steps = jnp.exp(jax.random.uniform(jax.random.fold_in(own, dim), (shards_of,), jnp.float32, smallest / len(pieces), top_value / len(pieces)))
        gain = gain * jnp.repeat(steps, dims[dim] // shards_of).reshape([-1 if axis == dim else 1 for axis in range(len(dims))])
    return gain


def profile(count, total, bound, slope):
    loads = [(1 << 20) // math.isqrt(standing ** slope) + 1 for standing in range(2, count + 1)]
    surplus, given = total - bound - (count - 1), [1] * (count - 1)
    while surplus > 0:
        candidates = [i for i in range(count - 1) if given[i] < bound]
        pool, remaining = sum([loads[i] for i in candidates]), surplus
        for i in candidates:
            extra = min(bound - given[i], max(1, remaining * loads[i] // pool), surplus)
            given[i] = given[i] + extra
            surplus = surplus - extra
    return np.array([bound] + given)


def ragged_sizes(rng, number_of, total, bound, slope):
    if number_of == 2:
        one = jax.random.randint(rng, (), max(1, total - bound), min(bound, total - 1) + 1)
        return jnp.stack([one, total - one])
    sizes = jnp.asarray(profile(number_of, total, bound, slope), jnp.int32)
    twos = (number_of - 1) // 2
    donor, sink = sizes[1:1 + 2 * twos:2], sizes[2:2 + 2 * twos:2]
    slack = jnp.minimum(donor - 1, bound - sink)
    shifted = jax.random.randint(jax.random.fold_in(rng, 1), (twos,), 0, 1 << 20) % (slack + 1)
    sizes = sizes.at[1:1 + 2 * twos:2].set(donor - shifted).at[2:2 + 2 * twos:2].set(sink + shifted)
    return sizes[jax.random.permutation(jax.random.fold_in(rng, 2), number_of)]


def gaussian(own_key, extent, spread, bound, cuts=(), kind=jnp.bfloat16):
    entries = jax.random.normal(own_key, extent, jnp.float32) * spread
    if len(cuts) > 0:
        entries = steps_of(own_key, extent, cuts, -0.22, 0.18) * entries
    return jnp.clip(entries, min=-bound, max=bound).astype(kind)


def setup_inputs(seed: int = 0) -> dict:
    keys = jax.random.split(jax.random.key(seed), 7)
    return {
        "master": draw_master(jax.random.fold_in(keys[6], 71), 0),
        "moment_one": gaussian(keys[1], (ROWS, W), 1.0, 6.0, ((0, 128),), jnp.float32),
        "moment_two": jnp.clip(jnp.exp(math.log(4.0) - 5.9914646 * jax.random.uniform(keys[2], (ROWS, W), jnp.float32) ** steps_of(keys[2], (ROWS, W), ((0, 128),), -0.2, 0.2)), 0.01, 4.0),
        "gradient": draw_gradient(jax.random.fold_in(keys[6], 71), 0),
        "partner": jax.random.permutation(keys[4], NDEV).astype(jnp.int32),
        "tensor_of_row": jnp.searchsorted(jnp.cumsum(ragged_sizes(keys[5], LAYERS, ROWS, 2 * ROWS // LAYERS, 1)), jnp.arange(ROWS), side="right").astype(jnp.int32),
    }


beta_one = 0.9
beta_two = 0.999
step_count = 10
adam_eps = 1e-06
trust_eps = 1e-06
learn_rate = 0.05
decay_rate = 0.01

def reference(master, moment_one, moment_two, gradient, partner, tensor_of_row):
    total_rows = master.shape[0]
    row_index = jnp.arange(total_rows, dtype=jnp.int32)
    owner = row_index // ROWS_DEV
    inside = row_index % ROWS_DEV
    rank = inside // BLOCK
    offset = inside % BLOCK
    place = (partner[rank] * ROWS_DEV + owner * BLOCK + offset).astype(jnp.int32)
    grad_rows = gradient[place]
    first = beta_one * moment_one + (1.0 - beta_one) * grad_rows
    second = beta_two * moment_two + (1.0 - beta_two) * grad_rows * grad_rows
    correct_one = 1.0 - beta_one ** step_count
    correct_two = 1.0 - beta_two ** step_count
    update = first / correct_one / (jnp.sqrt(second / correct_two) + adam_eps) + decay_rate * master
    weight_sq = jax.ops.segment_sum(lax.optimization_barrier(jnp.sum(master * master, axis=1)), tensor_of_row, num_segments=LAYERS)
    update_sq = jax.ops.segment_sum(lax.optimization_barrier(jnp.sum(update * update, axis=1)), tensor_of_row, num_segments=LAYERS)
    ratio = jnp.sqrt(weight_sq) / (jnp.sqrt(update_sq) + trust_eps)
    row_ratio = ratio[tensor_of_row]
    fresh = master - learn_rate * row_ratio[:, None] * update

    def settle(values):
        return jnp.zeros_like(values).at[place].set(values)
    return (settle(fresh), settle(first), settle(second))
```

```python
import functools

import jax
import jax.numpy as jnp
from jax import lax
from jax.experimental import pallas as pl
from jax.experimental.pallas import tpu as pltpu
from jax.sharding import Mesh
from jax.sharding import PartitionSpec as P

LAYERS = 8
GRP_SUB = ("grp", "sub")
LANES = 128
SUB = 8

beta_one = 0.9
beta_two = 0.999
step_count = 10
adam_eps = 1e-06
trust_eps = 1e-06
learn_rate = 0.05
decay_rate = 0.01
correct_one = 1.0 - beta_one**step_count
correct_two = 1.0 - beta_two**step_count


def pack_body(partner, master, one, two, out, lines, *, chunks, rows_step):
    pitch = 3 * chunks
    step = pl.program_id(0)

    def group(g, carry):
        for a, ref in enumerate((master, one, two)):
            for c in range(chunks):
                tile = ref[pl.ds(pl.multiple_of(g * SUB, SUB), SUB), c * LANES : (c + 1) * LANES]
                lines[pl.ds(a * chunks + c, SUB, stride=pitch), :] = tile
        for j in range(SUB):
            slot = partner[step * rows_step + g * SUB + j] * pitch
            for i in range(0, pitch, SUB):
                size = min(SUB, pitch - i)
                out[pl.ds(slot + i, size), :] = lines[j * pitch + i : j * pitch + i + size, :]
        return carry

    lax.fori_loop(0, rows_step // SUB, group, 0)


def adam_tiles(recv, grad, base, row, c, chunks):
    pitch = 3 * chunks
    weights = recv[pl.ds(base + c, SUB, stride=pitch), :]
    old_one = recv[pl.ds(base + chunks + c, SUB, stride=pitch), :]
    old_two = recv[pl.ds(base + 2 * chunks + c, SUB, stride=pitch), :]
    g = grad[pl.ds(row, SUB), c * LANES : (c + 1) * LANES]
    first = beta_one * old_one + (1.0 - beta_one) * g
    second = beta_two * old_two + (1.0 - beta_two) * g * g
    update = (first * (1.0 / correct_one)) / (
        jnp.sqrt(second * (1.0 / correct_two)) + adam_eps
    ) + decay_rate * weights
    return weights, first, second, update


def tensor_ids(ids, partner, device, row):
    mine = partner[...] == device
    return jnp.sum(jnp.where(mine, ids[pl.ds(row, SUB), :], 0), axis=1, keepdims=True)


def sums_body(device, partner, ids, recv, grad, out, acc, *, chunks, rows_step):
    pitch = 3 * chunks
    step = pl.program_id(0)

    @pl.when(step == 0)
    def _():
        acc[...] = jnp.zeros_like(acc)

    lane = lax.broadcasted_iota(jnp.int32, (SUB, LANES), 1)

    def group(g, carry):
        row = pl.multiple_of(g * SUB, SUB)
        update_sq = jnp.zeros((SUB, LANES), jnp.float32)
        weight_sq = jnp.zeros((SUB, LANES), jnp.float32)
        for c in range(chunks):
            weights, _, _, update = adam_tiles(recv, grad, g * SUB * pitch, row, c, chunks)
            update_sq += update * update
            weight_sq += weights * weights
        mine = tensor_ids(ids, partner, device[0], row)
        update_row = jnp.sum(update_sq, axis=1, keepdims=True)
        weight_row = jnp.sum(weight_sq, axis=1, keepdims=True)
        acc[...] += jnp.where(lane == mine, update_row, 0.0) + jnp.where(
            lane == mine + LAYERS, weight_row, 0.0
        )
        return carry

    lax.fori_loop(0, rows_step // SUB, group, 0)

    @pl.when(step == pl.num_programs(0) - 1)
    def _():
        total = jnp.sum(acc[...], axis=0, keepdims=True)
        out[...] = jnp.broadcast_to(total[None], out.shape)


def moments_body(recv, grad, first_out, second_out, update_out, weights_out, *, chunks, rows_step):
    pitch = 3 * chunks

    def group(g, carry):
        row = pl.multiple_of(g * SUB, SUB)
        for c in range(chunks):
            weights, first, second, update = adam_tiles(recv, grad, g * SUB * pitch, row, c, chunks)
            cols = slice(c * LANES, (c + 1) * LANES)
            first_out[pl.ds(row, SUB), cols] = first
            second_out[pl.ds(row, SUB), cols] = second
            update_out[pl.ds(row, SUB), cols] = update
            weights_out[pl.ds(row, SUB), cols] = weights
        return carry

    lax.fori_loop(0, rows_step // SUB, group, 0)


def master_body(device, partner, ids, sums, weights, update, out, *, chunks, rows_step):
    total = jnp.sum(sums[...], axis=0)
    update_sq = total
    weight_sq = pltpu.roll(jnp.broadcast_to(total, (SUB, LANES)), LANES - LAYERS, 1)[:1]
    ratio = jnp.sqrt(weight_sq) / (jnp.sqrt(update_sq) + trust_eps)
    lane = lax.broadcasted_iota(jnp.int32, (SUB, LANES), 1)

    def group(g, carry):
        row = pl.multiple_of(g * SUB, SUB)
        mine = tensor_ids(ids, partner, device[0], row)
        row_ratio = jnp.sum(jnp.where(lane == mine, ratio, 0.0), axis=1, keepdims=True)
        scale = learn_rate * row_ratio
        out[pl.ds(row, SUB), :] = weights[pl.ds(row, SUB), :] - scale * update[pl.ds(row, SUB), :]
        return carry

    lax.fori_loop(0, rows_step // SUB, group, 0)


def local(master, moment_one, moment_two, gradient, partner, tensor_of_row):
    rows, width = master.shape
    devices = lax.axis_size(GRP_SUB)
    chunks = width // LANES
    pitch = 3 * chunks
    steps = 4
    rows_step = rows // steps
    device = lax.axis_index(GRP_SUB).astype(jnp.int32).reshape(1)
    partner_row = partner.reshape(1, devices)
    ids = tensor_of_row.reshape(rows, devices)
    size = dict(chunks=chunks, rows_step=rows_step)
    row_spec = pl.BlockSpec((rows_step, width), lambda i: (i, 0))
    recv_spec = pl.BlockSpec((rows_step * pitch, LANES), lambda i: (i, 0))
    ids_spec = pl.BlockSpec((rows_step, devices), lambda i: (i, 0))
    whole = lambda *shape: pl.BlockSpec(shape, lambda i: (0,) * len(shape))
    scalars = pl.BlockSpec(memory_space=pltpu.SMEM)
    array = jax.ShapeDtypeStruct((rows, width), jnp.float32)

    packed = pl.pallas_call(
        functools.partial(pack_body, **size),
        grid=(steps,),
        in_specs=[scalars, row_spec, row_spec, row_spec],
        out_specs=whole(rows * pitch, LANES),
        out_shape=jax.ShapeDtypeStruct((rows * pitch, LANES), jnp.float32),
        scratch_shapes=[pltpu.VMEM((SUB * pitch, LANES), jnp.float32)],
        name="pack",
    )(partner, master, moment_one, moment_two)
    sent = packed.reshape(devices, 1, pitch * LANES)
    recv = lax.all_to_all(sent, GRP_SUB, split_axis=0, concat_axis=0, tiled=True)
    recv = recv.reshape(rows * pitch, LANES)

    sums = pl.pallas_call(
        functools.partial(sums_body, **size),
        grid=(steps,),
        in_specs=[scalars, whole(1, devices), ids_spec, recv_spec, row_spec],
        out_specs=whole(devices, 1, LANES),
        out_shape=jax.ShapeDtypeStruct((devices, 1, LANES), jnp.float32),
        scratch_shapes=[pltpu.VMEM((SUB, LANES), jnp.float32)],
        name="sums",
    )(device, partner_row, ids, recv, gradient)
    all_sums = lax.all_to_all(sums, GRP_SUB, split_axis=0, concat_axis=0, tiled=True)

    first, second, update, weights = pl.pallas_call(
        functools.partial(moments_body, **size),
        grid=(steps,),
        in_specs=[recv_spec, row_spec],
        out_specs=[row_spec] * 4,
        out_shape=[array] * 4,
        cost_estimate=pl.CostEstimate(flops=30_000_000, bytes_accessed=15_000_000, transcendentals=1_000_000),
        name="moments",
    )(recv, gradient)

    fresh = pl.pallas_call(
        functools.partial(master_body, **size),
        grid=(steps,),
        in_specs=[scalars, whole(1, devices), ids_spec, whole(devices, 1, LANES), row_spec, row_spec],
        out_specs=row_spec,
        out_shape=array,
        name="fresh",
    )(device, partner_row, ids, all_sums, weights, update)
    return (fresh, first, second)


def solution(mesh):
    rows = P(GRP_SUB, None)
    return jax.shard_map(
        local,
        mesh=mesh,
        in_specs=(rows, rows, rows, rows, P(), P()),
        out_specs=(rows, rows, rows),
        check_vma=False,
    )
```

```python
import functools

import jax
import jax.numpy as jnp
from jax import lax
from jax.experimental import pallas as pl
from jax.experimental.pallas import tpu as pltpu
from jax.sharding import Mesh
from jax.sharding import PartitionSpec as P

LAYERS = 8
GRP_SUB = ("grp", "sub")
LANES = 128
SUB = 8

beta_one = 0.9
beta_two = 0.999
step_count = 10
adam_eps = 1e-06
trust_eps = 1e-06
learn_rate = 0.05
decay_rate = 0.01
correct_one = 1.0 - beta_one**step_count
correct_two = 1.0 - beta_two**step_count


def pack_body(partner, master, one, two, out, rows_of, lines, arrived, *, chunks, parts):
    pitch = 3 * chunks
    part = master.shape[0] // parts
    groups = part // SUB

    def fetch(a, ref, p):
        rows = pl.ds(p * part, part)
        return pltpu.make_async_copy(ref.at[rows], rows_of.at[a, rows], arrived.at[a, p])

    for p in range(parts):
        for a, ref in enumerate((master, one, two)):
            fetch(a, ref, p).start()

    for p in range(parts):
        for a, ref in enumerate((master, one, two)):
            fetch(a, ref, p).wait()

        def group(g, carry, p=p):
            row = pl.multiple_of(p * part + g * SUB, SUB)
            for a in range(3):
                for c in range(chunks):
                    tile = rows_of[a, pl.ds(row, SUB), c * LANES : (c + 1) * LANES]
                    lines[pl.ds(a * chunks + c, SUB, stride=pitch), :] = tile
            for j in range(SUB):
                slot = partner[row + j] * pitch
                for i in range(0, pitch, SUB):
                    size = min(SUB, pitch - i)
                    out[pl.ds(slot + i, size), :] = lines[j * pitch + i : j * pitch + i + size, :]
            return carry

        lax.fori_loop(0, groups, group, 0)


def adam_tiles(recv, grad, base, row, c, chunks):
    pitch = 3 * chunks
    weights = recv[pl.ds(base + c, SUB, stride=pitch), :]
    old_one = recv[pl.ds(base + chunks + c, SUB, stride=pitch), :]
    old_two = recv[pl.ds(base + 2 * chunks + c, SUB, stride=pitch), :]
    g = grad[pl.ds(row, SUB), c * LANES : (c + 1) * LANES]
    first = beta_one * old_one + (1.0 - beta_one) * g
    second = beta_two * old_two + (1.0 - beta_two) * g * g
    update = (first * (1.0 / correct_one)) / (
        jnp.sqrt(second * (1.0 / correct_two)) + adam_eps
    ) + decay_rate * weights
    return weights, first, second, update


def tensor_ids(ids, partner, device, row):
    mine = partner[...] == device
    return jnp.sum(jnp.where(mine, ids[pl.ds(row, SUB), :], 0), axis=1, keepdims=True)


def sums_body(
    device, partner, ids, recv, grad, sums, first_out, second_out, update_out, weights_out, acc, *, chunks, rows_step
):
    pitch = 3 * chunks
    step = pl.program_id(0)

    @pl.when(step == 0)
    def _():
        acc[...] = jnp.zeros_like(acc)

    lane = lax.broadcasted_iota(jnp.int32, (SUB, LANES), 1)

    def group(g, carry):
        row = pl.multiple_of(g * SUB, SUB)
        kept = pl.multiple_of(step * rows_step + row, SUB)
        update_sq = jnp.zeros((SUB, LANES), jnp.float32)
        weight_sq = jnp.zeros((SUB, LANES), jnp.float32)
        for c in range(chunks):
            weights, first, second, update = adam_tiles(recv, grad, g * SUB * pitch, row, c, chunks)
            cols = slice(c * LANES, (c + 1) * LANES)
            first_out[pl.ds(row, SUB), cols] = first
            second_out[pl.ds(row, SUB), cols] = second
            update_out[pl.ds(kept, SUB), cols] = update
            weights_out[pl.ds(kept, SUB), cols] = weights
            update_sq += update * update
            weight_sq += weights * weights
        mine = tensor_ids(ids, partner, device[0], row)
        update_row = jnp.sum(update_sq, axis=1, keepdims=True)
        weight_row = jnp.sum(weight_sq, axis=1, keepdims=True)
        acc[...] += jnp.where(lane == mine, update_row, 0.0) + jnp.where(
            lane == mine + LAYERS, weight_row, 0.0
        )
        return carry

    lax.fori_loop(0, rows_step // SUB, group, 0)

    @pl.when(step == pl.num_programs(0) - 1)
    def _():
        total = jnp.sum(acc[...], axis=0, keepdims=True)
        sums[...] = jnp.broadcast_to(total[None], sums.shape)


def master_body(device, partner, ids, sums, weights, update, out, *, chunks, rows_step):
    total = jnp.sum(sums[...], axis=0)
    update_sq = total
    weight_sq = pltpu.roll(jnp.broadcast_to(total, (SUB, LANES)), LANES - LAYERS, 1)[:1]
    ratio = jnp.sqrt(weight_sq) / (jnp.sqrt(update_sq) + trust_eps)
    lane = lax.broadcasted_iota(jnp.int32, (SUB, LANES), 1)

    def group(g, carry):
        row = pl.multiple_of(g * SUB, SUB)
        mine = tensor_ids(ids, partner, device[0], row)
        row_ratio = jnp.sum(jnp.where(lane == mine, ratio, 0.0), axis=1, keepdims=True)
        scale = learn_rate * row_ratio
        out[pl.ds(row, SUB), :] = weights[pl.ds(row, SUB), :] - scale * update[pl.ds(row, SUB), :]
        return carry

    lax.fori_loop(0, rows_step // SUB, group, 0)


def local(master, moment_one, moment_two, gradient, partner, tensor_of_row):
    rows, width = master.shape
    devices = lax.axis_size(GRP_SUB)
    chunks = width // LANES
    pitch = 3 * chunks
    steps = 4
    rows_step = rows // steps
    device = lax.axis_index(GRP_SUB).astype(jnp.int32).reshape(1)
    partner_row = partner.reshape(1, devices)
    ids = tensor_of_row.reshape(rows, devices)
    size = dict(chunks=chunks, rows_step=rows_step)
    row_spec = pl.BlockSpec((rows_step, width), lambda i: (i, 0))
    recv_spec = pl.BlockSpec((rows_step * pitch, LANES), lambda i: (i, 0))
    ids_spec = pl.BlockSpec((rows_step, devices), lambda i: (i, 0))
    whole = lambda *shape: pl.BlockSpec(shape, lambda i: (0,) * len(shape))
    scalars = pl.BlockSpec(memory_space=pltpu.SMEM)
    array = jax.ShapeDtypeStruct((rows, width), jnp.float32)

    in_hbm = pl.BlockSpec(memory_space=pltpu.HBM)
    limit = pltpu.CompilerParams(vmem_limit_bytes=16 << 20)
    parts = 8
    packed = pl.pallas_call(
        functools.partial(pack_body, chunks=chunks, parts=parts),
        in_specs=[scalars, in_hbm, in_hbm, in_hbm],
        out_specs=pl.BlockSpec(memory_space=pltpu.VMEM),
        out_shape=jax.ShapeDtypeStruct((rows * pitch, LANES), jnp.float32),
        scratch_shapes=[
            pltpu.VMEM((3, rows, width), jnp.float32),
            pltpu.VMEM((SUB * pitch, LANES), jnp.float32),
            pltpu.SemaphoreType.DMA((3, parts)),
        ],
        compiler_params=limit,
        name="pack",
    )(*[pltpu.with_memory_space_constraint(v, pltpu.HBM) for v in (partner, master, moment_one, moment_two)])
    packed, device = lax.optimization_barrier((packed, device))
    sent = packed.reshape(devices, 1, pitch * LANES)
    recv = lax.all_to_all(sent, GRP_SUB, split_axis=0, concat_axis=0, tiled=True)
    recv = recv.reshape(rows * pitch, LANES)

    sums, first, second, update, weights = pl.pallas_call(
        functools.partial(sums_body, **size),
        grid=(steps,),
        in_specs=[scalars, whole(1, devices), ids_spec, recv_spec, row_spec],
        out_specs=[whole(devices, 1, LANES), row_spec, row_spec, whole(rows, width), whole(rows, width)],
        out_shape=[jax.ShapeDtypeStruct((devices, 1, LANES), jnp.float32)] + [array] * 4,
        scratch_shapes=[pltpu.VMEM((SUB, LANES), jnp.float32)],
        compiler_params=limit,
        name="sums",
    )(device, partner_row, ids, recv, gradient)
    all_sums = lax.all_to_all(sums, GRP_SUB, split_axis=0, concat_axis=0, tiled=True)

    fresh = pl.pallas_call(
        functools.partial(master_body, **size),
        grid=(steps,),
        in_specs=[scalars, whole(1, devices), ids_spec, whole(devices, 1, LANES), row_spec, row_spec],
        out_specs=row_spec,
        out_shape=array,
        compiler_params=limit,
        name="fresh",
    )(device, partner_row, ids, all_sums, weights, update)
    return (fresh, first, second)


def solution(mesh):
    rows = P(GRP_SUB, None)
    return jax.shard_map(
        local,
        mesh=mesh,
        in_specs=(rows, rows, rows, rows, P(), P()),
        out_specs=(rows, rows, rows),
        check_vma=False,
    )
```

```python
import functools

import jax
import jax.numpy as jnp
from jax import lax
from jax.experimental import pallas as pl
from jax.experimental.pallas import tpu as pltpu
from jax.sharding import PartitionSpec as P

LAYERS = 8
GRP_SUB = ("grp", "sub")
LANES = 128
SUB = 8
PARTS = 8

beta_one = 0.9
beta_two = 0.999
step_count = 10
adam_eps = 1e-06
trust_eps = 1e-06
learn_rate = 0.05
decay_rate = 0.01
correct_one = 1.0 - beta_one**step_count
correct_two = 1.0 - beta_two**step_count


def pack_body(
    partner_hbm, ids_hbm, master, one, two, out, mine, partner, ids, rows_of, lines, arrived, tables, *, chunks, per_grp
):
    pitch = 3 * chunks
    rows = master.shape[0]
    part = rows // PARTS

    def fetch(a, ref, p):
        span = pl.ds(p * part, part)
        return pltpu.make_async_copy(ref.at[span], rows_of.at[a, span], arrived.at[a, p])

    partner_copy = pltpu.make_async_copy(partner_hbm, partner, tables.at[0])
    ids_copy = pltpu.make_async_copy(ids_hbm, ids, tables.at[1])
    partner_copy.start()
    ids_copy.start()
    for p in range(PARTS):
        for a, ref in enumerate((master, one, two)):
            fetch(a, ref, p).start()

    partner_copy.wait()
    device = lax.axis_index("grp") * per_grp + lax.axis_index("sub")
    rank = jnp.int32(0)
    for n in range(rows):
        rank = jnp.where(partner[n] == device, n, rank)
    lane = lax.broadcasted_iota(jnp.int32, (SUB, LANES), 1)
    ids_copy.wait()
    for g in range(rows // SUB):
        span = slice(g * SUB, (g + 1) * SUB)
        chosen = jnp.sum(jnp.where(lane == rank, ids[span, :], 0), axis=1, keepdims=True)
        mine[span, :] = jnp.broadcast_to(chosen, (SUB, LANES))

    for p in range(PARTS):
        for a, ref in enumerate((master, one, two)):
            fetch(a, ref, p).wait()

        def group(g, carry, p=p):
            row = pl.multiple_of(p * part + g * SUB, SUB)
            for a in range(3):
                for c in range(chunks):
                    tile = rows_of[a, pl.ds(row, SUB), c * LANES : (c + 1) * LANES]
                    lines[pl.ds(a * chunks + c, SUB, stride=pitch), :] = tile
            for j in range(SUB):
                slot = partner[row + j] * pitch
                for i in range(0, pitch, SUB):
                    size = min(SUB, pitch - i)
                    out[pl.ds(slot + i, size), :] = lines[j * pitch + i : j * pitch + i + size, :]
            return carry

        lax.fori_loop(0, part // SUB, group, 0)


def adam_body(recv, grad, mine, first_hbm, second_hbm, sums, update_out, weights_out, first_out, second_out, left, *, chunks):
    pitch = 3 * chunks
    zero = jnp.zeros((SUB, LANES), jnp.float32)
    groups = grad.shape[0] // SUB

    def leave(g):
        span = pl.ds(pl.multiple_of(g * SUB, SUB), SUB)
        return (
            pltpu.make_async_copy(first_out.at[span], first_hbm.at[span], left.at[0, g]),
            pltpu.make_async_copy(second_out.at[span], second_hbm.at[span], left.at[1, g]),
        )

    def group(g, totals):
        row = pl.multiple_of(g * SUB, SUB)
        base = g * SUB * pitch
        update_sq, weight_sq = zero, zero
        for c in range(chunks):
            cols = slice(c * LANES, (c + 1) * LANES)
            weights = recv[pl.ds(base + c, SUB, stride=pitch), :]
            old_one = recv[pl.ds(base + chunks + c, SUB, stride=pitch), :]
            old_two = recv[pl.ds(base + 2 * chunks + c, SUB, stride=pitch), :]
            slope = grad[pl.ds(row, SUB), cols]
            first = beta_one * old_one + (1.0 - beta_one) * slope
            second = beta_two * old_two + (1.0 - beta_two) * slope * slope
            update = (first * (1.0 / correct_one)) / (
                jnp.sqrt(second * (1.0 / correct_two)) + adam_eps
            ) + decay_rate * weights
            first_out[pl.ds(row, SUB), cols] = first
            second_out[pl.ds(row, SUB), cols] = second
            update_out[pl.ds(row, SUB), cols] = update
            weights_out[pl.ds(row, SUB), cols] = weights
            update_sq += update * update
            weight_sq += weights * weights
        for copy in leave(g):
            copy.start()
        tensor = mine[pl.ds(row, SUB), :]
        masks = [tensor == t for t in range(LAYERS)]
        return tuple(
            total + jnp.where(masks[k % LAYERS], update_sq if k < LAYERS else weight_sq, 0.0)
            for k, total in enumerate(totals)
        )

    totals = lax.fori_loop(0, groups, group, (zero,) * (2 * LAYERS))
    lane = lax.broadcasted_iota(jnp.int32, (1, LANES), 1)
    line = jnp.zeros((1, LANES), jnp.float32)
    for k, total in enumerate(totals):
        value = jnp.sum(jnp.sum(total, axis=0, keepdims=True), axis=1, keepdims=True)
        line += jnp.where(lane == k, value, 0.0)
    sums[...] = jnp.broadcast_to(line, sums.shape)
    for g in range(groups):
        for copy in leave(g):
            copy.wait()


def master_body(sums, mine, weights, update, out, fresh, sent):
    rows = weights.shape[0]
    part = rows // PARTS
    total = jnp.broadcast_to(jnp.sum(sums[...], axis=0, keepdims=True), (SUB, LANES))
    weight_sq = pltpu.roll(total, LANES - LAYERS, 1)
    ratio = jnp.sqrt(weight_sq) / (jnp.sqrt(total) + trust_eps)
    lane = lax.broadcasted_iota(jnp.int32, (SUB, LANES), 1)
    scales = [
        jnp.broadcast_to(
            jnp.sum(jnp.where(lane == t, learn_rate * ratio, 0.0), axis=1, keepdims=True), (SUB, LANES)
        )
        for t in range(LAYERS)
    ]

    def leave(p):
        span = pl.ds(p * part, part)
        return pltpu.make_async_copy(fresh.at[span], out.at[span], sent.at[p])

    for p in range(PARTS):
        for g in range(part // SUB):
            span = slice(p * part + g * SUB, p * part + (g + 1) * SUB)
            tensor = mine[span, :]
            scale = scales[0]
            for t in range(1, LAYERS):
                scale = jnp.where(tensor == t, scales[t], scale)
            for c in range(0, weights.shape[1], LANES):
                cols = slice(c, c + LANES)
                fresh[span, cols] = weights[span, cols] - scale * update[span, cols]
        leave(p).start()
    for p in range(PARTS):
        leave(p).wait()


def local(master, moment_one, moment_two, gradient, partner, tensor_of_row):
    rows, width = master.shape
    devices = lax.axis_size(GRP_SUB)
    chunks = width // LANES
    pitch = 3 * chunks
    ids = tensor_of_row.reshape(rows, devices)
    array = jax.ShapeDtypeStruct((rows, width), jnp.float32)
    in_hbm = pl.BlockSpec(memory_space=pltpu.HBM)
    in_vmem = pl.BlockSpec(memory_space=pltpu.VMEM)
    limit = pltpu.CompilerParams(vmem_limit_bytes=16 << 20)
    hbm = lambda v: pltpu.with_memory_space_constraint(v, pltpu.HBM)

    packed, mine = pl.pallas_call(
        functools.partial(pack_body, chunks=chunks, per_grp=lax.axis_size("sub")),
        in_specs=[in_hbm] * 5,
        out_specs=[in_vmem] * 2,
        out_shape=[
            jax.ShapeDtypeStruct((rows * pitch, LANES), jnp.float32),
            jax.ShapeDtypeStruct((rows, LANES), jnp.int32),
        ],
        scratch_shapes=[
            pltpu.SMEM((devices,), jnp.int32),
            pltpu.VMEM((rows, devices), jnp.int32),
            pltpu.VMEM((3, rows, width), jnp.float32),
            pltpu.VMEM((SUB * pitch, LANES), jnp.float32),
            pltpu.SemaphoreType.DMA((3, PARTS)),
            pltpu.SemaphoreType.DMA((2,)),
        ],
        compiler_params=limit,
        name="pack",
    )(hbm(partner), hbm(ids), hbm(master), hbm(moment_one), hbm(moment_two))
    packed, mine = lax.optimization_barrier((packed, mine))
    sent = packed.reshape(devices, 1, pitch * LANES)
    recv = lax.all_to_all(sent, GRP_SUB, split_axis=0, concat_axis=0, tiled=True)
    recv = recv.reshape(rows * pitch, LANES)

    first, second, sums, update, weights = pl.pallas_call(
        functools.partial(adam_body, chunks=chunks),
        in_specs=[in_vmem] * 3,
        out_specs=[in_hbm] * 2 + [in_vmem] * 3,
        out_shape=[array] * 2 + [jax.ShapeDtypeStruct((devices, LANES), jnp.float32)] + [array] * 2,
        scratch_shapes=[pltpu.VMEM((rows, width), jnp.float32)] * 2
        + [pltpu.SemaphoreType.DMA((2, rows // SUB))],
        compiler_params=limit,
        name="adam",
    )(recv, gradient, mine)
    sums = lax.all_to_all(
        sums.reshape(devices, 1, LANES), GRP_SUB, split_axis=0, concat_axis=0, tiled=True
    ).reshape(devices, LANES)

    fresh = pl.pallas_call(
        master_body,
        in_specs=[in_vmem] * 4,
        out_specs=in_hbm,
        out_shape=array,
        scratch_shapes=[pltpu.VMEM((rows, width), jnp.float32), pltpu.SemaphoreType.DMA((PARTS,))],
        compiler_params=limit,
        name="fresh",
    )(sums, mine, weights, update)
    return (fresh, first, second)


def solution(mesh):
    rows = P(GRP_SUB, None)
    return jax.shard_map(
        local,
        mesh=mesh,
        in_specs=(rows, rows, rows, rows, P(), P()),
        out_specs=(rows, rows, rows),
        check_vma=False,
    )
```

```python
import functools

import jax
import jax.numpy as jnp
from jax import lax
from jax.experimental import pallas as pl
from jax.experimental.pallas import tpu as pltpu
from jax.sharding import PartitionSpec as P

LAYERS = 8
GRP_SUB = ("grp", "sub")
LANES = 128
SUB = 8
PARTS = 8
SHARES = (7, 5, 3, 1)

beta_one = 0.9
beta_two = 0.999
step_count = 10
adam_eps = 1e-06
trust_eps = 1e-06
learn_rate = 0.05
decay_rate = 0.01
correct_one = 1.0 - beta_one**step_count
correct_two = 1.0 - beta_two**step_count
root_scale = correct_one / correct_two**0.5


def pack_body(
    partner_hbm, ids_hbm, master, one, two, out, mine, partner, ids, rows_of, lines, arrived, tables, *, chunks, per_grp
):
    pitch = 3 * chunks
    rows = master.shape[0]
    unit = rows // sum(SHARES)
    starts = [unit * sum(SHARES[:p]) for p in range(len(SHARES))]

    def fetch(a, ref, p):
        span = pl.ds(starts[p], unit * SHARES[p])
        return pltpu.make_async_copy(ref.at[span], rows_of.at[a, span], arrived.at[a, p])

    partner_copy = pltpu.make_async_copy(partner_hbm, partner, tables.at[0])
    ids_copy = pltpu.make_async_copy(ids_hbm, ids, tables.at[1])
    partner_copy.start()
    ids_copy.start()
    for p in range(len(SHARES)):
        for a, ref in enumerate((master, one, two)):
            fetch(a, ref, p).start()

    partner_copy.wait()
    device = lax.axis_index("grp") * per_grp + lax.axis_index("sub")
    rank = jnp.int32(0)
    for n in range(rows):
        rank = jnp.where(partner[n] == device, n, rank)
    lane = lax.broadcasted_iota(jnp.int32, (SUB, LANES), 1)
    ids_copy.wait()
    for g in range(rows // SUB):
        span = slice(g * SUB, (g + 1) * SUB)
        chosen = jnp.sum(jnp.where(lane == rank, ids[span, :], 0), axis=1, keepdims=True)
        mine[span, :] = jnp.broadcast_to(chosen, (SUB, LANES))

    for p in range(len(SHARES)):
        for a, ref in enumerate((master, one, two)):
            fetch(a, ref, p).wait()

        def group(g, carry, p=p):
            row = pl.multiple_of(starts[p] + g * SUB, SUB)
            for a in range(3):
                for c in range(chunks):
                    tile = rows_of[a, pl.ds(row, SUB), c * LANES : (c + 1) * LANES]
                    lines[pl.ds(a * chunks + c, SUB, stride=pitch), :] = tile
            for j in range(SUB):
                slot = partner[row + j] * pitch
                for i in range(0, pitch, SUB):
                    size = min(SUB, pitch - i)
                    out[pl.ds(slot + i, size), :] = lines[j * pitch + i : j * pitch + i + size, :]
            return carry

        lax.fori_loop(0, unit * SHARES[p] // SUB, group, 0)


def adam_body(recv, grad, mine, first_hbm, second_hbm, sums, update_out, first_out, second_out, left, *, chunks):
    pitch = 3 * chunks
    zero = jnp.zeros((SUB, LANES), jnp.float32)
    groups = grad.shape[0] // SUB

    def leave(g):
        span = pl.ds(pl.multiple_of(g * SUB, SUB), SUB)
        return (
            pltpu.make_async_copy(first_out.at[span], first_hbm.at[span], left.at[0, g]),
            pltpu.make_async_copy(second_out.at[span], second_hbm.at[span], left.at[1, g]),
        )

    def group(g, totals):
        row = pl.multiple_of(g * SUB, SUB)
        base = g * SUB * pitch
        update_sq, weight_sq = zero, zero
        for c in range(chunks):
            cols = slice(c * LANES, (c + 1) * LANES)
            weights = recv[pl.ds(base + c, SUB, stride=pitch), :]
            old_one = recv[pl.ds(base + chunks + c, SUB, stride=pitch), :]
            old_two = recv[pl.ds(base + 2 * chunks + c, SUB, stride=pitch), :]
            slope = grad[pl.ds(row, SUB), cols]
            first = beta_one * old_one + (1.0 - beta_one) * slope
            second = beta_two * old_two + (1.0 - beta_two) * slope * slope
            root = second * lax.rsqrt(second)
            update = first / (root * root_scale + correct_one * adam_eps) + decay_rate * weights
            first_out[pl.ds(row, SUB), cols] = first
            second_out[pl.ds(row, SUB), cols] = second
            update_out[pl.ds(row, SUB), cols] = update
            update_sq += update * update
            weight_sq += weights * weights
        for copy in leave(g):
            copy.start()
        tensor = mine[pl.ds(row, SUB), :]
        masks = [tensor == t for t in range(LAYERS)]
        return tuple(
            total + jnp.where(masks[k % LAYERS], update_sq if k < LAYERS else weight_sq, 0.0)
            for k, total in enumerate(totals)
        )

    totals = lax.fori_loop(0, groups, group, (zero,) * (2 * LAYERS))
    lane = lax.broadcasted_iota(jnp.int32, (1, LANES), 1)
    line = jnp.zeros((1, LANES), jnp.float32)
    for k, total in enumerate(totals):
        value = jnp.sum(jnp.sum(total, axis=0, keepdims=True), axis=1, keepdims=True)
        line += jnp.where(lane == k, value, 0.0)
    sums[...] = jnp.broadcast_to(line, sums.shape)
    for g in range(groups):
        for copy in leave(g):
            copy.wait()


def master_body(sums, mine, recv, update, out, fresh, sent, *, chunks):
    rows = update.shape[0]
    pitch = 3 * chunks
    part = rows // PARTS
    total = jnp.broadcast_to(jnp.sum(sums[...], axis=0, keepdims=True), (SUB, LANES))
    weight_sq = pltpu.roll(total, LANES - LAYERS, 1)
    ratio = jnp.sqrt(weight_sq) / (jnp.sqrt(total) + trust_eps)
    lane = lax.broadcasted_iota(jnp.int32, (SUB, LANES), 1)
    scales = [
        jnp.broadcast_to(
            jnp.sum(jnp.where(lane == t, learn_rate * ratio, 0.0), axis=1, keepdims=True), (SUB, LANES)
        )
        for t in range(LAYERS)
    ]

    def leave(p):
        span = pl.ds(p * part, part)
        return pltpu.make_async_copy(fresh.at[span], out.at[span], sent.at[p])

    for p in range(PARTS):
        for g in range(part // SUB):
            span = slice(p * part + g * SUB, p * part + (g + 1) * SUB)
            tensor = mine[span, :]
            scale = scales[0]
            for t in range(1, LAYERS):
                scale = jnp.where(tensor == t, scales[t], scale)
            for c in range(chunks):
                cols = slice(c * LANES, (c + 1) * LANES)
                weights = recv[pl.ds(span.start * pitch + c, SUB, stride=pitch), :]
                fresh[span, cols] = weights - scale * update[span, cols]
        leave(p).start()
    for p in range(PARTS):
        leave(p).wait()


def local(master, moment_one, moment_two, gradient, partner, tensor_of_row):
    rows, width = master.shape
    devices = lax.axis_size(GRP_SUB)
    chunks = width // LANES
    pitch = 3 * chunks
    ids = tensor_of_row.reshape(rows, devices)
    array = jax.ShapeDtypeStruct((rows, width), jnp.float32)
    in_hbm = pl.BlockSpec(memory_space=pltpu.HBM)
    in_vmem = pl.BlockSpec(memory_space=pltpu.VMEM)
    limit = pltpu.CompilerParams(vmem_limit_bytes=16 << 20)
    hbm = lambda v: pltpu.with_memory_space_constraint(v, pltpu.HBM)

    packed, mine = pl.pallas_call(
        functools.partial(pack_body, chunks=chunks, per_grp=lax.axis_size("sub")),
        in_specs=[in_hbm] * 5,
        out_specs=[in_vmem] * 2,
        out_shape=[
            jax.ShapeDtypeStruct((rows * pitch, LANES), jnp.float32),
            jax.ShapeDtypeStruct((rows, LANES), jnp.int32),
        ],
        scratch_shapes=[
            pltpu.SMEM((devices,), jnp.int32),
            pltpu.VMEM((rows, devices), jnp.int32),
            pltpu.VMEM((3, rows, width), jnp.float32),
            pltpu.VMEM((SUB * pitch, LANES), jnp.float32),
            pltpu.SemaphoreType.DMA((3, len(SHARES))),
            pltpu.SemaphoreType.DMA((2,)),
        ],
        compiler_params=limit,
        name="pack",
    )(hbm(partner), hbm(ids), hbm(master), hbm(moment_one), hbm(moment_two))
    packed, mine = lax.optimization_barrier((packed, mine))
    sent = packed.reshape(devices, 1, pitch * LANES)
    recv = lax.all_to_all(sent, GRP_SUB, split_axis=0, concat_axis=0, tiled=True)
    recv = recv.reshape(rows * pitch, LANES)

    first, second, sums, update = pl.pallas_call(
        functools.partial(adam_body, chunks=chunks),
        in_specs=[in_vmem] * 3,
        out_specs=[in_hbm] * 2 + [in_vmem] * 2,
        out_shape=[array] * 2 + [jax.ShapeDtypeStruct((devices, LANES), jnp.float32), array],
        scratch_shapes=[pltpu.VMEM((rows, width), jnp.float32)] * 2
        + [pltpu.SemaphoreType.DMA((2, rows // SUB))],
        compiler_params=limit,
        name="adam",
    )(recv, gradient, mine)
    sums = lax.all_to_all(
        sums.reshape(devices, 1, LANES), GRP_SUB, split_axis=0, concat_axis=0, tiled=True
    ).reshape(devices, LANES)

    fresh = pl.pallas_call(
        functools.partial(master_body, chunks=chunks),
        in_specs=[in_vmem] * 4,
        out_specs=in_hbm,
        out_shape=array,
        scratch_shapes=[pltpu.VMEM((rows, width), jnp.float32), pltpu.SemaphoreType.DMA((PARTS,))],
        compiler_params=limit,
        name="fresh",
    )(sums, mine, recv, update)
    return (fresh, first, second)


def solution(mesh):
    rows = P(GRP_SUB, None)
    return jax.shard_map(
        local,
        mesh=mesh,
        in_specs=(rows, rows, rows, rows, P(), P()),
        out_specs=(rows, rows, rows),
        check_vma=False,
    )
```

```python
import functools

import jax
import jax.numpy as jnp
from jax import lax
from jax.experimental import pallas as pl
from jax.experimental.pallas import tpu as pltpu
from jax.sharding import PartitionSpec as P

LAYERS = 8
GRP_SUB = ("grp", "sub")
LANES = 128
SUB = 8
PARTS = 8
SHARES = (8, 8)

beta_one = 0.9
beta_two = 0.999
step_count = 10
adam_eps = 1e-06
trust_eps = 1e-06
learn_rate = 0.05
decay_rate = 0.01
correct_one = 1.0 - beta_one**step_count
correct_two = 1.0 - beta_two**step_count
root_scale = correct_one / correct_two**0.5


def pack_body(
    partner_hbm, ids_hbm, master, one, two, out, mine, partner, ids, rows_of, lines, arrived, tables, *, chunks, per_grp
):
    pitch = 3 * chunks
    rows = master.shape[0]
    unit = rows // sum(SHARES)
    starts = [unit * sum(SHARES[:p]) for p in range(len(SHARES))]

    def fetch(a, ref, p):
        span = pl.ds(starts[p], unit * SHARES[p])
        return pltpu.make_async_copy(ref.at[span], rows_of.at[a, span], arrived.at[a, p])

    partner_copy = pltpu.make_async_copy(partner_hbm, partner, tables.at[0])
    ids_copy = pltpu.make_async_copy(ids_hbm, ids, tables.at[1])
    partner_copy.start()
    ids_copy.start()
    for p in range(len(SHARES)):
        for a, ref in enumerate((master, one, two)):
            fetch(a, ref, p).start()

    partner_copy.wait()
    device = lax.axis_index("grp") * per_grp + lax.axis_index("sub")
    rank = jnp.int32(0)
    for n in range(rows):
        rank = jnp.where(partner[n] == device, n, rank)
    lane = lax.broadcasted_iota(jnp.int32, (SUB, LANES), 1)
    ids_copy.wait()
    for g in range(rows // SUB):
        span = slice(g * SUB, (g + 1) * SUB)
        chosen = jnp.sum(jnp.where(lane == rank, ids[span, :], 0), axis=1, keepdims=True)
        mine[span, :] = jnp.broadcast_to(chosen, (SUB, LANES))

    for p in range(len(SHARES)):
        for a, ref in enumerate((master, one, two)):
            fetch(a, ref, p).wait()

        def group(g, carry, p=p):
            row = pl.multiple_of(starts[p] + g * SUB, SUB)
            for a in range(3):
                for c in range(chunks):
                    tile = rows_of[a, pl.ds(row, SUB), c * LANES : (c + 1) * LANES]
                    lines[pl.ds(a * chunks + c, SUB, stride=pitch), :] = tile
            for j in range(SUB):
                slot = partner[row + j] * pitch
                for i in range(0, pitch, SUB):
                    size = min(SUB, pitch - i)
                    out[pl.ds(slot + i, size), :] = lines[j * pitch + i : j * pitch + i + size, :]
            return carry

        lax.fori_loop(0, unit * SHARES[p] // SUB, group, 0)


def adam_body(recv, grad, mine, first_hbm, second_hbm, sums, update_out, first_out, second_out, left, *, chunks):
    pitch = 3 * chunks
    zero = jnp.zeros((SUB, LANES), jnp.float32)
    groups = grad.shape[0] // SUB

    def leave(g):
        span = pl.ds(pl.multiple_of(g * SUB, SUB), SUB)
        return (
            pltpu.make_async_copy(first_out.at[span], first_hbm.at[span], left.at[0, g]),
            pltpu.make_async_copy(second_out.at[span], second_hbm.at[span], left.at[1, g]),
        )

    def group(g, totals):
        row = pl.multiple_of(g * SUB, SUB)
        base = g * SUB * pitch
        update_sq, weight_sq = zero, zero
        for c in range(chunks):
            cols = slice(c * LANES, (c + 1) * LANES)
            weights = recv[pl.ds(base + c, SUB, stride=pitch), :]
            old_one = recv[pl.ds(base + chunks + c, SUB, stride=pitch), :]
            old_two = recv[pl.ds(base + 2 * chunks + c, SUB, stride=pitch), :]
            slope = grad[pl.ds(row, SUB), cols]
            first = beta_one * old_one + (1.0 - beta_one) * slope
            second = beta_two * old_two + (1.0 - beta_two) * slope * slope
            root = second * lax.rsqrt(second)
            update = first / (root * root_scale + correct_one * adam_eps) + decay_rate * weights
            first_out[pl.ds(row, SUB), cols] = first
            second_out[pl.ds(row, SUB), cols] = second
            update_out[pl.ds(row, SUB), cols] = update
            update_sq += update * update
            weight_sq += weights * weights
        for copy in leave(g):
            copy.start()
        tensor = mine[pl.ds(row, SUB), :]
        masks = [tensor == t for t in range(LAYERS)]
        return tuple(
            total + jnp.where(masks[k % LAYERS], update_sq if k < LAYERS else weight_sq, 0.0)
            for k, total in enumerate(totals)
        )

    totals = lax.fori_loop(0, groups, group, (zero,) * (2 * LAYERS))
    lane = lax.broadcasted_iota(jnp.int32, (1, LANES), 1)
    line = jnp.zeros((1, LANES), jnp.float32)
    for k, total in enumerate(totals):
        value = jnp.sum(jnp.sum(total, axis=0, keepdims=True), axis=1, keepdims=True)
        line += jnp.where(lane == k, value, 0.0)
    sums[...] = jnp.broadcast_to(line, sums.shape)
    for g in range(groups):
        for copy in leave(g):
            copy.wait()


def master_body(sums, mine, recv, update, out, fresh, sent, *, chunks):
    rows = update.shape[0]
    pitch = 3 * chunks
    part = rows // PARTS
    total = jnp.broadcast_to(jnp.sum(sums[...], axis=0, keepdims=True), (SUB, LANES))
    weight_sq = pltpu.roll(total, LANES - LAYERS, 1)
    ratio = jnp.sqrt(weight_sq) / (jnp.sqrt(total) + trust_eps)
    lane = lax.broadcasted_iota(jnp.int32, (SUB, LANES), 1)
    scales = [
        jnp.broadcast_to(
            jnp.sum(jnp.where(lane == t, learn_rate * ratio, 0.0), axis=1, keepdims=True), (SUB, LANES)
        )
        for t in range(LAYERS)
    ]

    def leave(p):
        span = pl.ds(p * part, part)
        return pltpu.make_async_copy(fresh.at[span], out.at[span], sent.at[p])

    for p in range(PARTS):
        for g in range(part // SUB):
            span = slice(p * part + g * SUB, p * part + (g + 1) * SUB)
            tensor = mine[span, :]
            scale = scales[0]
            for t in range(1, LAYERS):
                scale = jnp.where(tensor == t, scales[t], scale)
            for c in range(chunks):
                cols = slice(c * LANES, (c + 1) * LANES)
                weights = recv[pl.ds(span.start * pitch + c, SUB, stride=pitch), :]
                fresh[span, cols] = weights - scale * update[span, cols]
        leave(p).start()
    for p in range(PARTS):
        leave(p).wait()


def local(master, moment_one, moment_two, gradient, partner, tensor_of_row):
    rows, width = master.shape
    devices = lax.axis_size(GRP_SUB)
    chunks = width // LANES
    pitch = 3 * chunks
    ids = tensor_of_row.reshape(rows, devices)
    array = jax.ShapeDtypeStruct((rows, width), jnp.float32)
    in_hbm = pl.BlockSpec(memory_space=pltpu.HBM)
    in_vmem = pl.BlockSpec(memory_space=pltpu.VMEM)
    limit = pltpu.CompilerParams(vmem_limit_bytes=16 << 20)
    hbm = lambda v: pltpu.with_memory_space_constraint(v, pltpu.HBM)

    packed, mine = pl.pallas_call(
        functools.partial(pack_body, chunks=chunks, per_grp=lax.axis_size("sub")),
        in_specs=[in_hbm] * 5,
        out_specs=[in_vmem] * 2,
        out_shape=[
            jax.ShapeDtypeStruct((rows * pitch, LANES), jnp.float32),
            jax.ShapeDtypeStruct((rows, LANES), jnp.int32),
        ],
        scratch_shapes=[
            pltpu.SMEM((devices,), jnp.int32),
            pltpu.VMEM((rows, devices), jnp.int32),
            pltpu.VMEM((3, rows, width), jnp.float32),
            pltpu.VMEM((SUB * pitch, LANES), jnp.float32),
            pltpu.SemaphoreType.DMA((3, len(SHARES))),
            pltpu.SemaphoreType.DMA((2,)),
        ],
        compiler_params=limit,
        name="pack",
    )(hbm(partner), hbm(ids), hbm(master), hbm(moment_one), hbm(moment_two))
    packed, mine = lax.optimization_barrier((packed, mine))
    sent = packed.reshape(devices, 1, pitch * LANES)
    recv = lax.all_to_all(sent, GRP_SUB, split_axis=0, concat_axis=0, tiled=True)
    recv = recv.reshape(rows * pitch, LANES)

    first, second, sums, update = pl.pallas_call(
        functools.partial(adam_body, chunks=chunks),
        in_specs=[in_vmem] * 3,
        out_specs=[in_hbm] * 2 + [in_vmem] * 2,
        out_shape=[array] * 2 + [jax.ShapeDtypeStruct((devices, LANES), jnp.float32), array],
        scratch_shapes=[pltpu.VMEM((rows, width), jnp.float32)] * 2
        + [pltpu.SemaphoreType.DMA((2, rows // SUB))],
        compiler_params=limit,
        name="adam",
    )(recv, gradient, mine)
    sums = lax.all_to_all(
        sums.reshape(devices, 1, LANES), GRP_SUB, split_axis=0, concat_axis=0, tiled=True
    ).reshape(devices, LANES)

    fresh = pl.pallas_call(
        functools.partial(master_body, chunks=chunks),
        in_specs=[in_vmem] * 4,
        out_specs=in_hbm,
        out_shape=array,
        scratch_shapes=[pltpu.VMEM((rows, width), jnp.float32), pltpu.SemaphoreType.DMA((PARTS,))],
        compiler_params=limit,
        name="fresh",
    )(sums, mine, recv, update)
    return (fresh, first, second)


def solution(mesh):
    rows = P(GRP_SUB, None)
    return jax.shard_map(
        local,
        mesh=mesh,
        in_specs=(rows, rows, rows, rows, P(), P()),
        out_specs=(rows, rows, rows),
        check_vma=False,
    )
```

```python
import functools

import jax
import jax.numpy as jnp
from jax import lax
from jax.experimental import pallas as pl
from jax.experimental.pallas import tpu as pltpu
from jax.sharding import PartitionSpec as P

LAYERS = 8
GRP_SUB = ("grp", "sub")
LANES = 128
SUB = 8
PARTS = 8
SHARES = (8, 5, 3)
URGENCY = (0, 1, 1)

beta_one = 0.9
beta_two = 0.999
step_count = 10
adam_eps = 1e-06
trust_eps = 1e-06
learn_rate = 0.05
decay_rate = 0.01
correct_one = 1.0 - beta_one**step_count
correct_two = 1.0 - beta_two**step_count
root_scale = correct_one / correct_two**0.5


def pack_body(
    partner_hbm, ids_hbm, master, one, two, out, mine, partner, ids, rows_of, lines, arrived, tables, *, chunks, per_grp
):
    pitch = 3 * chunks
    rows = master.shape[0]
    unit = rows // sum(SHARES)
    starts = [unit * sum(SHARES[:p]) for p in range(len(SHARES))]

    def fetch(a, ref, p):
        span = pl.ds(starts[p], unit * SHARES[p])
        return pltpu.make_async_copy(ref.at[span], rows_of.at[a, span], arrived.at[a, p])

    partner_copy = pltpu.make_async_copy(partner_hbm, partner, tables.at[0])
    ids_copy = pltpu.make_async_copy(ids_hbm, ids, tables.at[1])
    partner_copy.start()
    ids_copy.start()
    for p in range(len(SHARES)):
        for a, ref in enumerate((master, one, two)):
            fetch(a, ref, p).start(priority=URGENCY[p])

    partner_copy.wait()
    device = lax.axis_index("grp") * per_grp + lax.axis_index("sub")
    rank = jnp.int32(0)
    for n in range(rows):
        rank = jnp.where(partner[n] == device, n, rank)
    lane = lax.broadcasted_iota(jnp.int32, (SUB, LANES), 1)
    ids_copy.wait()
    for g in range(rows // SUB):
        span = slice(g * SUB, (g + 1) * SUB)
        chosen = jnp.sum(jnp.where(lane == rank, ids[span, :], 0), axis=1, keepdims=True)
        mine[span, :] = jnp.broadcast_to(chosen, (SUB, LANES))

    for p in range(len(SHARES)):
        for a, ref in enumerate((master, one, two)):
            fetch(a, ref, p).wait()

        def group(g, carry, p=p):
            row = pl.multiple_of(starts[p] + g * SUB, SUB)
            for a in range(3):
                for c in range(chunks):
                    tile = rows_of[a, pl.ds(row, SUB), c * LANES : (c + 1) * LANES]
                    lines[pl.ds(a * chunks + c, SUB, stride=pitch), :] = tile
            for j in range(SUB):
                slot = partner[row + j] * pitch
                for i in range(0, pitch, SUB):
                    size = min(SUB, pitch - i)
                    out[pl.ds(slot + i, size), :] = lines[j * pitch + i : j * pitch + i + size, :]
            return carry

        lax.fori_loop(0, unit * SHARES[p] // SUB, group, 0)


def adam_body(recv, grad, mine, first_hbm, second_hbm, sums, update_out, first_out, second_out, left, *, chunks):
    pitch = 3 * chunks
    zero = jnp.zeros((SUB, LANES), jnp.float32)
    groups = grad.shape[0] // SUB

    def leave(g):
        span = pl.ds(pl.multiple_of(g * SUB, SUB), SUB)
        return (
            pltpu.make_async_copy(first_out.at[span], first_hbm.at[span], left.at[0, g]),
            pltpu.make_async_copy(second_out.at[span], second_hbm.at[span], left.at[1, g]),
        )

    def group(g, totals):
        row = pl.multiple_of(g * SUB, SUB)
        base = g * SUB * pitch
        update_sq, weight_sq = zero, zero
        for c in range(chunks):
            cols = slice(c * LANES, (c + 1) * LANES)
            weights = recv[pl.ds(base + c, SUB, stride=pitch), :]
            old_one = recv[pl.ds(base + chunks + c, SUB, stride=pitch), :]
            old_two = recv[pl.ds(base + 2 * chunks + c, SUB, stride=pitch), :]
            slope = grad[pl.ds(row, SUB), cols]
            first = beta_one * old_one + (1.0 - beta_one) * slope
            second = beta_two * old_two + (1.0 - beta_two) * slope * slope
            root = second * lax.rsqrt(second)
            update = first / (root * root_scale + correct_one * adam_eps) + decay_rate * weights
            first_out[pl.ds(row, SUB), cols] = first
            second_out[pl.ds(row, SUB), cols] = second
            update_out[pl.ds(row, SUB), cols] = update
            update_sq += update * update
            weight_sq += weights * weights
        for copy in leave(g):
            copy.start()
        tensor = mine[pl.ds(row, SUB), :]
        masks = [tensor == t for t in range(LAYERS)]
        return tuple(
            total + jnp.where(masks[k % LAYERS], update_sq if k < LAYERS else weight_sq, 0.0)
            for k, total in enumerate(totals)
        )

    totals = lax.fori_loop(0, groups, group, (zero,) * (2 * LAYERS))
    lane = lax.broadcasted_iota(jnp.int32, (1, LANES), 1)
    line = jnp.zeros((1, LANES), jnp.float32)
    for k, total in enumerate(totals):
        value = jnp.sum(jnp.sum(total, axis=0, keepdims=True), axis=1, keepdims=True)
        line += jnp.where(lane == k, value, 0.0)
    sums[...] = jnp.broadcast_to(line, sums.shape)
    for g in range(groups):
        for copy in leave(g):
            copy.wait()


def master_body(sums, mine, recv, update, out, fresh, sent, *, chunks):
    rows = update.shape[0]
    pitch = 3 * chunks
    part = rows // PARTS
    total = jnp.broadcast_to(jnp.sum(sums[...], axis=0, keepdims=True), (SUB, LANES))
    weight_sq = pltpu.roll(total, LANES - LAYERS, 1)
    ratio = jnp.sqrt(weight_sq) / (jnp.sqrt(total) + trust_eps)
    lane = lax.broadcasted_iota(jnp.int32, (SUB, LANES), 1)
    scales = [
        jnp.broadcast_to(
            jnp.sum(jnp.where(lane == t, learn_rate * ratio, 0.0), axis=1, keepdims=True), (SUB, LANES)
        )
        for t in range(LAYERS)
    ]

    def leave(p):
        span = pl.ds(p * part, part)
        return pltpu.make_async_copy(fresh.at[span], out.at[span], sent.at[p])

    for p in range(PARTS):
        for g in range(part // SUB):
            span = slice(p * part + g * SUB, p * part + (g + 1) * SUB)
            tensor = mine[span, :]
            scale = scales[0]
            for t in range(1, LAYERS):
                scale = jnp.where(tensor == t, scales[t], scale)
            for c in range(chunks):
                cols = slice(c * LANES, (c + 1) * LANES)
                weights = recv[pl.ds(span.start * pitch + c, SUB, stride=pitch), :]
                fresh[span, cols] = weights - scale * update[span, cols]
        leave(p).start()
    for p in range(PARTS):
        leave(p).wait()


def local(master, moment_one, moment_two, gradient, partner, tensor_of_row):
    rows, width = master.shape
    devices = lax.axis_size(GRP_SUB)
    chunks = width // LANES
    pitch = 3 * chunks
    ids = tensor_of_row.reshape(rows, devices)
    array = jax.ShapeDtypeStruct((rows, width), jnp.float32)
    in_hbm = pl.BlockSpec(memory_space=pltpu.HBM)
    in_vmem = pl.BlockSpec(memory_space=pltpu.VMEM)
    limit = pltpu.CompilerParams(vmem_limit_bytes=16 << 20)
    hbm = lambda v: pltpu.with_memory_space_constraint(v, pltpu.HBM)

    packed, mine = pl.pallas_call(
        functools.partial(pack_body, chunks=chunks, per_grp=lax.axis_size("sub")),
        in_specs=[in_hbm] * 5,
        out_specs=[in_vmem] * 2,
        out_shape=[
            jax.ShapeDtypeStruct((rows * pitch, LANES), jnp.float32),
            jax.ShapeDtypeStruct((rows, LANES), jnp.int32),
        ],
        scratch_shapes=[
            pltpu.SMEM((devices,), jnp.int32),
            pltpu.VMEM((rows, devices), jnp.int32),
            pltpu.VMEM((3, rows, width), jnp.float32),
            pltpu.VMEM((SUB * pitch, LANES), jnp.float32),
            pltpu.SemaphoreType.DMA((3, len(SHARES))),
            pltpu.SemaphoreType.DMA((2,)),
        ],
        compiler_params=limit,
        name="pack",
    )(hbm(partner), hbm(ids), hbm(master), hbm(moment_one), hbm(moment_two))
    packed, mine = lax.optimization_barrier((packed, mine))
    sent = packed.reshape(devices, 1, pitch * LANES)
    recv = lax.all_to_all(sent, GRP_SUB, split_axis=0, concat_axis=0, tiled=True)
    recv = recv.reshape(rows * pitch, LANES)

    first, second, sums, update = pl.pallas_call(
        functools.partial(adam_body, chunks=chunks),
        in_specs=[in_vmem] * 3,
        out_specs=[in_hbm] * 2 + [in_vmem] * 2,
        out_shape=[array] * 2 + [jax.ShapeDtypeStruct((devices, LANES), jnp.float32), array],
        scratch_shapes=[pltpu.VMEM((rows, width), jnp.float32)] * 2
        + [pltpu.SemaphoreType.DMA((2, rows // SUB))],
        compiler_params=limit,
        name="adam",
    )(recv, gradient, mine)
    sums = lax.all_to_all(
        sums.reshape(devices, 1, LANES), GRP_SUB, split_axis=0, concat_axis=0, tiled=True
    ).reshape(devices, LANES)

    fresh = pl.pallas_call(
        functools.partial(master_body, chunks=chunks),
        in_specs=[in_vmem] * 4,
        out_specs=in_hbm,
        out_shape=array,
        scratch_shapes=[pltpu.VMEM((rows, width), jnp.float32), pltpu.SemaphoreType.DMA((PARTS,))],
        compiler_params=limit,
        name="fresh",
    )(sums, mine, recv, update)
    return (fresh, first, second)


def solution(mesh):
    rows = P(GRP_SUB, None)
    return jax.shard_map(
        local,
        mesh=mesh,
        in_specs=(rows, rows, rows, rows, P(), P()),
        out_specs=(rows, rows, rows),
        check_vma=False,
    )
```

```python
import functools

import jax
import jax.numpy as jnp
from jax import lax
from jax.experimental import pallas as pl
from jax.experimental.pallas import tpu as pltpu
from jax.sharding import PartitionSpec as P

LAYERS = 8
GRP_SUB = ("grp", "sub")
LANES = 128
SUB = 8
PARTS = 8
SHARES = (8, 5, 3)
URGENCY = (0, 1, 1)
LATE = 6

beta_one = 0.9
beta_two = 0.999
step_count = 10
adam_eps = 1e-06
trust_eps = 1e-06
learn_rate = 0.05
decay_rate = 0.01
correct_one = 1.0 - beta_one**step_count
correct_two = 1.0 - beta_two**step_count
root_scale = correct_one / correct_two**0.5


def pack_body(
    partner_hbm, ids_hbm, master, one, two, out, mine, partner, ids, rows_of, lines, arrived, tables, *, chunks, per_grp
):
    pitch = 3 * chunks
    rows = master.shape[0]
    unit = rows // sum(SHARES)
    starts = [unit * sum(SHARES[:p]) for p in range(len(SHARES))]

    def fetch(a, ref, p):
        span = pl.ds(starts[p], unit * SHARES[p])
        return pltpu.make_async_copy(ref.at[span], rows_of.at[a, span], arrived.at[a, p])

    partner_copy = pltpu.make_async_copy(partner_hbm, partner, tables.at[0])
    ids_copy = pltpu.make_async_copy(ids_hbm, ids, tables.at[1])
    partner_copy.start()
    ids_copy.start()
    for p in range(len(SHARES)):
        for a, ref in enumerate((master, one, two)):
            fetch(a, ref, p).start(priority=URGENCY[p])

    partner_copy.wait()
    device = lax.axis_index("grp") * per_grp + lax.axis_index("sub")
    rank = jnp.int32(0)
    for n in range(rows):
        rank = jnp.where(partner[n] == device, n, rank)
    lane = lax.broadcasted_iota(jnp.int32, (SUB, LANES), 1)
    ids_copy.wait()
    for g in range(rows // SUB):
        span = slice(g * SUB, (g + 1) * SUB)
        chosen = jnp.sum(jnp.where(lane == rank, ids[span, :], 0), axis=1, keepdims=True)
        mine[span, :] = jnp.broadcast_to(chosen, (SUB, LANES))

    for p in range(len(SHARES)):
        for a, ref in enumerate((master, one, two)):
            fetch(a, ref, p).wait()

        def group(g, carry, p=p):
            row = pl.multiple_of(starts[p] + g * SUB, SUB)
            for a in range(3):
                for c in range(chunks):
                    tile = rows_of[a, pl.ds(row, SUB), c * LANES : (c + 1) * LANES]
                    lines[pl.ds(a * chunks + c, SUB, stride=pitch), :] = tile
            for j in range(SUB):
                slot = partner[row + j] * pitch
                for i in range(0, pitch, SUB):
                    size = min(SUB, pitch - i)
                    out[pl.ds(slot + i, size), :] = lines[j * pitch + i : j * pitch + i + size, :]
            return carry

        lax.fori_loop(0, unit * SHARES[p] // SUB, group, 0)


def adam_body(recv, grad, mine, first_hbm, second_hbm, sums, update_out, first_late, second_late, first_out, second_out, left, *, chunks):
    pitch = 3 * chunks
    zero = jnp.zeros((SUB, LANES), jnp.float32)
    groups = grad.shape[0] // SUB
    early = groups - LATE

    def leave(g):
        span = pl.ds(pl.multiple_of(g * SUB, SUB), SUB)
        return (
            pltpu.make_async_copy(first_out.at[span], first_hbm.at[span], left.at[0, g]),
            pltpu.make_async_copy(second_out.at[span], second_hbm.at[span], left.at[1, g]),
        )

    def group(g, totals, late):
        row = pl.multiple_of(g * SUB, SUB)
        kept = pl.multiple_of((g - early) * SUB, SUB) if late else row
        base = g * SUB * pitch
        update_sq, weight_sq = zero, zero
        for c in range(chunks):
            cols = slice(c * LANES, (c + 1) * LANES)
            weights = recv[pl.ds(base + c, SUB, stride=pitch), :]
            old_one = recv[pl.ds(base + chunks + c, SUB, stride=pitch), :]
            old_two = recv[pl.ds(base + 2 * chunks + c, SUB, stride=pitch), :]
            slope = grad[pl.ds(row, SUB), cols]
            first = beta_one * old_one + (1.0 - beta_one) * slope
            second = beta_two * old_two + (1.0 - beta_two) * slope * slope
            root = second * lax.rsqrt(second)
            update = first / (root * root_scale + correct_one * adam_eps) + decay_rate * weights
            (first_late if late else first_out)[pl.ds(kept, SUB), cols] = first
            (second_late if late else second_out)[pl.ds(kept, SUB), cols] = second
            update_out[pl.ds(row, SUB), cols] = update
            update_sq += update * update
            weight_sq += weights * weights
        if not late:
            for copy in leave(g):
                copy.start()
        tensor = mine[pl.ds(row, SUB), :]
        masks = [tensor == t for t in range(LAYERS)]
        return tuple(
            total + jnp.where(masks[k % LAYERS], update_sq if k < LAYERS else weight_sq, 0.0)
            for k, total in enumerate(totals)
        )

    totals = lax.fori_loop(0, early, functools.partial(group, late=False), (zero,) * (2 * LAYERS))
    totals = lax.fori_loop(early, groups, functools.partial(group, late=True), totals)
    lane = lax.broadcasted_iota(jnp.int32, (1, LANES), 1)
    line = jnp.zeros((1, LANES), jnp.float32)
    for k, total in enumerate(totals):
        value = jnp.sum(jnp.sum(total, axis=0, keepdims=True), axis=1, keepdims=True)
        line += jnp.where(lane == k, value, 0.0)
    sums[...] = jnp.broadcast_to(line, sums.shape)
    for g in range(early):
        for copy in leave(g):
            copy.wait()


def master_body(
    sums,
    mine,
    recv,
    update,
    first_late,
    second_late,
    first_in,
    second_in,
    out,
    first_out,
    second_out,
    fresh,
    sent,
    late,
    *,
    chunks,
):
    rows = update.shape[0]
    rest = pl.ds(rows - LATE * SUB, LATE * SUB)
    late_copies = [
        pltpu.make_async_copy(source, whole.at[rest], late.at[k])
        for k, (source, whole) in enumerate(((first_late, first_out), (second_late, second_out)))
    ]
    for copy in late_copies:
        copy.start()
    pitch = 3 * chunks
    part = rows // PARTS
    total = jnp.broadcast_to(jnp.sum(sums[...], axis=0, keepdims=True), (SUB, LANES))
    weight_sq = pltpu.roll(total, LANES - LAYERS, 1)
    ratio = jnp.sqrt(weight_sq) / (jnp.sqrt(total) + trust_eps)
    lane = lax.broadcasted_iota(jnp.int32, (SUB, LANES), 1)
    scales = [
        jnp.broadcast_to(
            jnp.sum(jnp.where(lane == t, learn_rate * ratio, 0.0), axis=1, keepdims=True), (SUB, LANES)
        )
        for t in range(LAYERS)
    ]

    def leave(p):
        span = pl.ds(p * part, part)
        return pltpu.make_async_copy(fresh.at[span], out.at[span], sent.at[p])

    for p in range(PARTS):
        for g in range(part // SUB):
            span = slice(p * part + g * SUB, p * part + (g + 1) * SUB)
            tensor = mine[span, :]
            scale = scales[0]
            for t in range(1, LAYERS):
                scale = jnp.where(tensor == t, scales[t], scale)
            for c in range(chunks):
                cols = slice(c * LANES, (c + 1) * LANES)
                weights = recv[pl.ds(span.start * pitch + c, SUB, stride=pitch), :]
                fresh[span, cols] = weights - scale * update[span, cols]
        leave(p).start()
    for copy in late_copies:
        copy.wait()
    for p in range(PARTS):
        leave(p).wait()


def local(master, moment_one, moment_two, gradient, partner, tensor_of_row):
    rows, width = master.shape
    devices = lax.axis_size(GRP_SUB)
    chunks = width // LANES
    pitch = 3 * chunks
    ids = tensor_of_row.reshape(rows, devices)
    array = jax.ShapeDtypeStruct((rows, width), jnp.float32)
    in_hbm = pl.BlockSpec(memory_space=pltpu.HBM)
    in_vmem = pl.BlockSpec(memory_space=pltpu.VMEM)
    limit = pltpu.CompilerParams(vmem_limit_bytes=16 << 20)
    hbm = lambda v: pltpu.with_memory_space_constraint(v, pltpu.HBM)

    packed, mine = pl.pallas_call(
        functools.partial(pack_body, chunks=chunks, per_grp=lax.axis_size("sub")),
        in_specs=[in_hbm] * 5,
        out_specs=[in_vmem] * 2,
        out_shape=[
            jax.ShapeDtypeStruct((rows * pitch, LANES), jnp.float32),
            jax.ShapeDtypeStruct((rows, LANES), jnp.int32),
        ],
        scratch_shapes=[
            pltpu.SMEM((devices,), jnp.int32),
            pltpu.VMEM((rows, devices), jnp.int32),
            pltpu.VMEM((3, rows, width), jnp.float32),
            pltpu.VMEM((SUB * pitch, LANES), jnp.float32),
            pltpu.SemaphoreType.DMA((3, len(SHARES))),
            pltpu.SemaphoreType.DMA((2,)),
        ],
        compiler_params=limit,
        name="pack",
    )(hbm(partner), hbm(ids), hbm(master), hbm(moment_one), hbm(moment_two))
    packed, mine = lax.optimization_barrier((packed, mine))
    sent = packed.reshape(devices, 1, pitch * LANES)
    recv = lax.all_to_all(sent, GRP_SUB, split_axis=0, concat_axis=0, tiled=True)
    recv = recv.reshape(rows * pitch, LANES)

    late = jax.ShapeDtypeStruct((LATE * SUB, width), jnp.float32)
    first, second, sums, update, first_late, second_late = pl.pallas_call(
        functools.partial(adam_body, chunks=chunks),
        in_specs=[in_vmem] * 3,
        out_specs=[in_hbm] * 2 + [in_vmem] * 4,
        out_shape=[array] * 2 + [jax.ShapeDtypeStruct((devices, LANES), jnp.float32), array] + [late] * 2,
        scratch_shapes=[pltpu.VMEM((rows - LATE * SUB, width), jnp.float32)] * 2
        + [pltpu.SemaphoreType.DMA((2, rows // SUB - LATE))],
        compiler_params=limit,
        name="adam",
    )(recv, gradient, mine)
    sums = lax.all_to_all(
        sums.reshape(devices, 1, LANES), GRP_SUB, split_axis=0, concat_axis=0, tiled=True
    ).reshape(devices, LANES)

    fresh, first, second = pl.pallas_call(
        functools.partial(master_body, chunks=chunks),
        in_specs=[in_vmem] * 6 + [in_hbm] * 2,
        out_specs=[in_hbm] * 3,
        out_shape=[array] * 3,
        input_output_aliases={6: 1, 7: 2},
        scratch_shapes=[
            pltpu.VMEM((rows, width), jnp.float32),
            pltpu.SemaphoreType.DMA((PARTS,)),
            pltpu.SemaphoreType.DMA((2,)),
        ],
        compiler_params=limit,
        name="fresh",
    )(sums, mine, recv, update, first_late, second_late, hbm(first), hbm(second))
    return (fresh, first, second)


def solution(mesh):
    rows = P(GRP_SUB, None)
    return jax.shard_map(
        local,
        mesh=mesh,
        in_specs=(rows, rows, rows, rows, P(), P()),
        out_specs=(rows, rows, rows),
        check_vma=False,
    )
```

```python
import functools

import jax
import jax.numpy as jnp
from jax import lax
from jax.experimental import pallas as pl
from jax.experimental.pallas import tpu as pltpu
from jax.sharding import PartitionSpec as P

LAYERS = 8
GRP_SUB = ("grp", "sub")
LANES = 128
SUB = 8
PARTS = 8
SHARES = (8, 5, 3)
URGENCY = (0, 1, 1)
LATE = 6

beta_one = 0.9
beta_two = 0.999
step_count = 10
adam_eps = 1e-06
trust_eps = 1e-06
learn_rate = 0.05
decay_rate = 0.01
correct_one = 1.0 - beta_one**step_count
correct_two = 1.0 - beta_two**step_count
root_scale = correct_one / correct_two**0.5


def pack_body(
    partner_hbm, ids_hbm, master, one, two, out, mine, partner, ids, rows_of, lines, arrived, tables, *, chunks, per_grp
):
    pitch = 3 * chunks
    rows = master.shape[0]
    unit = rows // sum(SHARES)
    starts = [unit * sum(SHARES[:p]) for p in range(len(SHARES))]

    def fetch(a, ref, p):
        span = pl.ds(starts[p], unit * SHARES[p])
        return pltpu.make_async_copy(ref.at[span], rows_of.at[a, span], arrived.at[a, p])

    partner_copy = pltpu.make_async_copy(partner_hbm, partner, tables.at[0])
    ids_copy = pltpu.make_async_copy(ids_hbm, ids, tables.at[1])
    partner_copy.start()
    ids_copy.start()
    for p in range(len(SHARES)):
        for a, ref in enumerate((master, one, two)):
            fetch(a, ref, p).start(priority=URGENCY[p])

    partner_copy.wait()
    device = lax.axis_index("grp") * per_grp + lax.axis_index("sub")
    rank = jnp.int32(0)
    for n in range(rows):
        rank = jnp.where(partner[n] == device, n, rank)
    lane = lax.broadcasted_iota(jnp.int32, (SUB, LANES), 1)
    ids_copy.wait()
    for g in range(rows // SUB):
        span = slice(g * SUB, (g + 1) * SUB)
        chosen = jnp.sum(jnp.where(lane == rank, ids[span, :], 0), axis=1, keepdims=True)
        mine[span, :] = jnp.broadcast_to(chosen, (SUB, LANES))

    for p in range(len(SHARES)):
        for a, ref in enumerate((master, one, two)):
            fetch(a, ref, p).wait()

        def group(g, carry, p=p):
            row = pl.multiple_of(starts[p] + g * SUB, SUB)
            for a in range(3):
                for c in range(chunks):
                    tile = rows_of[a, pl.ds(row, SUB), c * LANES : (c + 1) * LANES]
                    lines[pl.ds(a * chunks + c, SUB, stride=pitch), :] = tile
            for j in range(SUB):
                slot = partner[row + j] * pitch
                for i in range(0, pitch, SUB):
                    size = min(SUB, pitch - i)
                    out[pl.ds(slot + i, size), :] = lines[j * pitch + i : j * pitch + i + size, :]
            return carry

        lax.fori_loop(0, unit * SHARES[p] // SUB, group, 0)


def adam_body(recv, grad, mine, first_hbm, second_hbm, sums, update_out, first_late, second_late, first_out, second_out, left, *, chunks):
    pitch = 3 * chunks
    zero = jnp.zeros((SUB, LANES), jnp.float32)
    groups = grad.shape[0] // SUB
    early = groups - LATE

    def leave(g):
        span = pl.ds(pl.multiple_of(g * SUB, SUB), SUB)
        return (
            pltpu.make_async_copy(first_out.at[span], first_hbm.at[span], left.at[0, g]),
            pltpu.make_async_copy(second_out.at[span], second_hbm.at[span], left.at[1, g]),
        )

    def group(g, totals, late):
        row = pl.multiple_of(g * SUB, SUB)
        kept = pl.multiple_of((g - early) * SUB, SUB) if late else row
        base = g * SUB * pitch
        update_sq, weight_sq = zero, zero
        for c in range(chunks):
            cols = slice(c * LANES, (c + 1) * LANES)
            weights = recv[pl.ds(base + c, SUB, stride=pitch), :]
            old_one = recv[pl.ds(base + chunks + c, SUB, stride=pitch), :]
            old_two = recv[pl.ds(base + 2 * chunks + c, SUB, stride=pitch), :]
            slope = grad[pl.ds(row, SUB), cols]
            first = beta_one * old_one + (1.0 - beta_one) * slope
            second = beta_two * old_two + (1.0 - beta_two) * slope * slope
            root = second * lax.rsqrt(second)
            update = first / (root * root_scale + correct_one * adam_eps) + decay_rate * weights
            (first_late if late else first_out)[pl.ds(kept, SUB), cols] = first
            (second_late if late else second_out)[pl.ds(kept, SUB), cols] = second
            update_out[pl.ds(row, SUB), cols] = update
            update_sq += update * update
            weight_sq += weights * weights
        if not late:
            for copy in leave(g):
                copy.start()
        tensor = mine[pl.ds(row, SUB), :]
        masks = [tensor == t for t in range(LAYERS)]
        return tuple(
            total + jnp.where(masks[k % LAYERS], update_sq if k < LAYERS else weight_sq, 0.0)
            for k, total in enumerate(totals)
        )

    totals = lax.fori_loop(0, early, functools.partial(group, late=False), (zero,) * (2 * LAYERS))
    totals = lax.fori_loop(early, groups, functools.partial(group, late=True), totals)
    lane = lax.broadcasted_iota(jnp.int32, (SUB, LANES), 1)
    sub = lax.broadcasted_iota(jnp.int32, (SUB, LANES), 0)
    placed = zero
    for first_lane in (0, LAYERS):
        stacked = zero
        for t in range(LAYERS):
            stacked = jnp.where(sub == t, jnp.sum(totals[first_lane + t], axis=0, keepdims=True), stacked)
        values = jnp.sum(stacked, axis=1, keepdims=True)
        placed += jnp.where(lane == sub + first_lane, values, 0.0)
    line = jnp.sum(placed, axis=0, keepdims=True)
    sums[...] = jnp.broadcast_to(line, sums.shape)
    for g in range(early):
        for copy in leave(g):
            copy.wait()


def master_body(
    sums,
    mine,
    recv,
    update,
    first_late,
    second_late,
    first_in,
    second_in,
    out,
    first_out,
    second_out,
    fresh,
    sent,
    late,
    *,
    chunks,
):
    rows = update.shape[0]
    rest = pl.ds(rows - LATE * SUB, LATE * SUB)
    late_copies = [
        pltpu.make_async_copy(source, whole.at[rest], late.at[k])
        for k, (source, whole) in enumerate(((first_late, first_out), (second_late, second_out)))
    ]
    for copy in late_copies:
        copy.start()
    pitch = 3 * chunks
    part = rows // PARTS
    total = jnp.broadcast_to(jnp.sum(sums[...], axis=0, keepdims=True), (SUB, LANES))
    weight_sq = pltpu.roll(total, LANES - LAYERS, 1)
    ratio = jnp.sqrt(weight_sq) / (jnp.sqrt(total) + trust_eps)
    lane = lax.broadcasted_iota(jnp.int32, (SUB, LANES), 1)
    scales = [
        jnp.broadcast_to(
            jnp.sum(jnp.where(lane == t, learn_rate * ratio, 0.0), axis=1, keepdims=True), (SUB, LANES)
        )
        for t in range(LAYERS)
    ]

    def leave(p):
        span = pl.ds(p * part, part)
        return pltpu.make_async_copy(fresh.at[span], out.at[span], sent.at[p])

    for p in range(PARTS):
        for g in range(part // SUB):
            span = slice(p * part + g * SUB, p * part + (g + 1) * SUB)
            tensor = mine[span, :]
            scale = scales[0]
            for t in range(1, LAYERS):
                scale = jnp.where(tensor == t, scales[t], scale)
            for c in range(chunks):
                cols = slice(c * LANES, (c + 1) * LANES)
                weights = recv[pl.ds(span.start * pitch + c, SUB, stride=pitch), :]
                fresh[span, cols] = weights - scale * update[span, cols]
        leave(p).start()
    for copy in late_copies:
        copy.wait()
    for p in range(PARTS):
        leave(p).wait()


def local(master, moment_one, moment_two, gradient, partner, tensor_of_row):
    rows, width = master.shape
    devices = lax.axis_size(GRP_SUB)
    chunks = width // LANES
    pitch = 3 * chunks
    ids = tensor_of_row.reshape(rows, devices)
    array = jax.ShapeDtypeStruct((rows, width), jnp.float32)
    in_hbm = pl.BlockSpec(memory_space=pltpu.HBM)
    in_vmem = pl.BlockSpec(memory_space=pltpu.VMEM)
    limit = pltpu.CompilerParams(vmem_limit_bytes=16 << 20)
    hbm = lambda v: pltpu.with_memory_space_constraint(v, pltpu.HBM)

    packed, mine = pl.pallas_call(
        functools.partial(pack_body, chunks=chunks, per_grp=lax.axis_size("sub")),
        in_specs=[in_hbm] * 5,
        out_specs=[in_vmem] * 2,
        out_shape=[
            jax.ShapeDtypeStruct((rows * pitch, LANES), jnp.float32),
            jax.ShapeDtypeStruct((rows, LANES), jnp.int32),
        ],
        scratch_shapes=[
            pltpu.SMEM((devices,), jnp.int32),
            pltpu.VMEM((rows, devices), jnp.int32),
            pltpu.VMEM((3, rows, width), jnp.float32),
            pltpu.VMEM((SUB * pitch, LANES), jnp.float32),
            pltpu.SemaphoreType.DMA((3, len(SHARES))),
            pltpu.SemaphoreType.DMA((2,)),
        ],
        compiler_params=limit,
        name="pack",
    )(hbm(partner), hbm(ids), hbm(master), hbm(moment_one), hbm(moment_two))
    packed, mine = lax.optimization_barrier((packed, mine))
    sent = packed.reshape(devices, 1, pitch * LANES)
    recv = lax.all_to_all(sent, GRP_SUB, split_axis=0, concat_axis=0, tiled=True)
    recv = recv.reshape(rows * pitch, LANES)

    late = jax.ShapeDtypeStruct((LATE * SUB, width), jnp.float32)
    first, second, sums, update, first_late, second_late = pl.pallas_call(
        functools.partial(adam_body, chunks=chunks),
        in_specs=[in_vmem] * 3,
        out_specs=[in_hbm] * 2 + [in_vmem] * 4,
        out_shape=[array] * 2 + [jax.ShapeDtypeStruct((devices, LANES), jnp.float32), array] + [late] * 2,
        scratch_shapes=[pltpu.VMEM((rows - LATE * SUB, width), jnp.float32)] * 2
        + [pltpu.SemaphoreType.DMA((2, rows // SUB - LATE))],
        compiler_params=limit,
        name="adam",
    )(recv, gradient, mine)
    sums = lax.all_to_all(
        sums.reshape(devices, 1, LANES), GRP_SUB, split_axis=0, concat_axis=0, tiled=True
    ).reshape(devices, LANES)

    fresh, first, second = pl.pallas_call(
        functools.partial(master_body, chunks=chunks),
        in_specs=[in_vmem] * 6 + [in_hbm] * 2,
        out_specs=[in_hbm] * 3,
        out_shape=[array] * 3,
        input_output_aliases={6: 1, 7: 2},
        scratch_shapes=[
            pltpu.VMEM((rows, width), jnp.float32),
            pltpu.SemaphoreType.DMA((PARTS,)),
            pltpu.SemaphoreType.DMA((2,)),
        ],
        compiler_params=limit,
        name="fresh",
    )(sums, mine, recv, update, first_late, second_late, hbm(first), hbm(second))
    return (fresh, first, second)


def solution(mesh):
    rows = P(GRP_SUB, None)
    return jax.shard_map(
        local,
        mesh=mesh,
        in_specs=(rows, rows, rows, rows, P(), P()),
        out_specs=(rows, rows, rows),
        check_vma=False,
    )
```
